16 devices in a mesh: dp: 2 (over y, z), tp: 8 (over x, core).
Axes of the slice: x: 4, y: 2, z: 1, core: 2. Of those that a mesh axis runs over, the one named last changes fastest.
The devices are a block of a 4x4x8 slice.
Arguments:
- hidden_in: bfloat16 [256, 5120], P(('dp', 'tp')), parts along dimension 0
- attn_norm: bfloat16 [5120], replicated
- mlp_norm: bfloat16 [5120], replicated
- w_query: bfloat16 [5120, 40, 128], P(None, 'tp')
- w_key: bfloat16 [5120, 8, 128], replicated
- w_value: bfloat16 [5120, 8, 128], replicated
- w_out: bfloat16 [40, 128, 5120], P('tp')
- w_gate: bfloat16 [5120, 17408], P(None, 'tp')
- w_up: bfloat16 [5120, 17408], P(None, 'tp')
- w_down: bfloat16 [17408, 5120], P('tp')
Outputs:
- output 1: bfloat16 [256, 5120], P(('dp', 'tp')), parts along dimension 0
- output 2: bfloat16 [256, 8, 128], P('dp', 'tp'), parts along dimension 0
- output 3: bfloat16 [256, 8, 128], P('dp', 'tp'), parts along dimension 0
There are 2 independent parts. The reference program is written for one: setup_inputs(seed, part) draws one part's arguments, and reference() takes and returns one part's arrays. A program takes and returns all parts, laid end to end along the dimension named above; an argument that names none is the same for every part.
All inputs are finite; a program needn't handle non-finite values.
Results may differ from the reference program's by a relative error of at most 0.0170683.
Values are sent between devices in bfloat16 or wider.
A program may use at most 768 MiB of HBM per device.

```python
import jax
import jax.numpy as jnp
from jax import lax

TOKENS = 128
DIM = 5120
HEADS = 40
KV_HEADS = 8
HEAD = 128
FF = 17408
KV_SLOTS = 8
Q_BLOCK = min(128, TOKENS)


def setup_inputs(seed: int = 0, part: int = 0) -> dict:
    key_list = jax.random.split(jax.random.key(seed), 10)
    hidden_key = jax.random.fold_in(key_list[0], part)
    inner_width = HEADS * HEAD
    attn_gain = 1.5 * (TOKENS / 64) ** 0.25
    hidden = jax.random.normal(hidden_key, (TOKENS, DIM), jnp.float32)
    attn_norm = jax.random.uniform(key_list[1], (DIM,), jnp.float32, 0.5, 1.5)
    mlp_norm = jax.random.uniform(key_list[2], (DIM,), jnp.float32, 0.5, 1.5)
    w_query = jax.random.normal(key_list[3], (DIM, HEADS, HEAD), jnp.float32) * (1.5 * DIM ** -0.5)
    w_key = jax.random.normal(key_list[4], (DIM, KV_HEADS, HEAD), jnp.float32) * DIM ** -0.5
    w_value = jax.random.normal(key_list[5], (DIM, KV_HEADS, HEAD), jnp.float32) * DIM ** -0.5
    w_out = jax.random.normal(key_list[6], (HEADS, HEAD, DIM), jnp.float32) * (attn_gain * inner_width ** -0.5)
    w_gate = jax.random.normal(key_list[7], (DIM, FF), jnp.float32) * DIM ** -0.5
    w_up = jax.random.normal(key_list[8], (DIM, FF), jnp.float32) * DIM ** -0.5
    w_down = jax.random.normal(key_list[9], (FF, DIM), jnp.float32) * (1.5 * FF ** -0.5)
    return dict(hidden_in=hidden.astype(jnp.bfloat16), attn_norm=attn_norm.astype(jnp.bfloat16), mlp_norm=mlp_norm.astype(jnp.bfloat16), w_query=w_query.astype(jnp.bfloat16), w_key=w_key.astype(jnp.bfloat16), w_value=w_value.astype(jnp.bfloat16), w_out=w_out.astype(jnp.bfloat16), w_gate=w_gate.astype(jnp.bfloat16), w_up=w_up.astype(jnp.bfloat16), w_down=w_down.astype(jnp.bfloat16))


def rms_norm(rows_in, gain_vec):
    rows_f = rows_in.astype(jnp.float32)
    mean_sq = jnp.mean(rows_f * rows_f, axis=-1, keepdims=True)
    return (rows_f * lax.rsqrt(mean_sq + 1e-5) * gain_vec.astype(jnp.float32)).astype(jnp.bfloat16)


def apply_rope(heads_f, positions):
    head_dim = heads_f.shape[-1]
    half_dim = head_dim // 2
    inv_freq = 1.0 / (500000.0 ** (jnp.arange(half_dim).astype(jnp.float32) * (2.0 / head_dim)))
    angles = positions[:, None] * inv_freq[None, :]
    cosine = jnp.cos(angles)[:, None, :]
    sine_val = jnp.sin(angles)[:, None, :]
    first_half = heads_f[..., :half_dim]
    second_half = heads_f[..., half_dim:]
    return jnp.concatenate([first_half * cosine - second_half * sine_val, second_half * cosine + first_half * sine_val], axis=-1)


def reference(hidden_in, attn_norm, mlp_norm, w_query, w_key, w_value, w_out, w_gate, w_up, w_down):
    group_size = HEADS // KV_HEADS
    positions = jnp.arange(TOKENS).astype(jnp.float32)
    normed = rms_norm(hidden_in, attn_norm)
    q_proj = jnp.dot(normed, w_query.reshape(DIM, HEADS * HEAD), preferred_element_type=jnp.float32).reshape(TOKENS, HEADS, HEAD)
    k_proj = jnp.dot(normed, w_key.reshape(DIM, KV_HEADS * HEAD), preferred_element_type=jnp.float32).reshape(TOKENS, KV_HEADS, HEAD)
    v_proj = jnp.dot(normed, w_value.reshape(DIM, KV_HEADS * HEAD), preferred_element_type=jnp.float32).astype(jnp.bfloat16).reshape(TOKENS, KV_HEADS, HEAD)
    q_rot = apply_rope(q_proj, positions).astype(jnp.bfloat16)
    k_rot = apply_rope(k_proj, positions).astype(jnp.bfloat16)
    q_blocks = q_rot.reshape(TOKENS // Q_BLOCK, Q_BLOCK, KV_HEADS, group_size, HEAD)
    key_pos = jnp.arange(TOKENS)
    k_float = k_rot.astype(jnp.float32)
    v_float = v_proj.astype(jnp.float32)

    def one_block(block_args):
        q_block, block_idx = block_args
        scores = jnp.einsum("qgrd,kgd->grqk", q_block.astype(jnp.float32), k_float) * (HEAD ** -0.5)
        query_pos = block_idx * Q_BLOCK + jnp.arange(Q_BLOCK)
        visible = key_pos[None, :] <= query_pos[:, None]
        scores = jnp.where(visible, scores, -1e30)
        probs_bf = jax.nn.softmax(scores, axis=-1).astype(jnp.bfloat16)
        block_out = jnp.einsum("grqk,kgd->qgrd", probs_bf.astype(jnp.float32), v_float)
        return block_out.astype(jnp.bfloat16)

    attn_out = lax.map(one_block, (q_blocks, jnp.arange(TOKENS // Q_BLOCK)))
    attn_flat = attn_out.reshape(TOKENS, HEADS * HEAD)
    attn_res = jnp.dot(attn_flat, w_out.reshape(HEADS * HEAD, DIM), preferred_element_type=jnp.float32)
    resid_mid = (hidden_in.astype(jnp.float32) + attn_res).astype(jnp.bfloat16)
    normed_mlp = rms_norm(resid_mid, mlp_norm)
    gate_proj = jnp.dot(normed_mlp, w_gate, preferred_element_type=jnp.float32)
    up_proj = jnp.dot(normed_mlp, w_up, preferred_element_type=jnp.float32)
    mlp_act = (jax.nn.silu(gate_proj) * up_proj).astype(jnp.bfloat16)
    mlp_res = jnp.dot(mlp_act, w_down, preferred_element_type=jnp.float32)
    hidden_out = (resid_mid.astype(jnp.float32) + mlp_res).astype(jnp.bfloat16)
    k_cache = jnp.repeat(k_rot, KV_SLOTS // KV_HEADS, axis=1)
    v_cache = jnp.repeat(v_proj, KV_SLOTS // KV_HEADS, axis=1)
    return (hidden_out, k_cache, v_cache)
```

```python
import functools

import jax
import jax.numpy as jnp
import numpy as np
from jax import lax
from jax.experimental import pallas as pl
from jax.experimental.pallas import tpu as pltpu
from jax.sharding import PartitionSpec as P

BF = jnp.bfloat16
F32 = jnp.float32
KC = 1024
RAW = 640
N_SLOTS = 9


def dot(a, b):
    return jnp.dot(a, b, preferred_element_type=F32)


def spans(width, step):
    return [(lo, min(step, width - lo)) for lo in range(0, width, step)]


def kernel(eps, hid_hbm, an_hbm, mn_hbm, cos_hbm, sin_hbm, wq_hbm, wk_hbm, wv_hbm, wo_hbm, wg_hbm, wu_hbm, wd_hbm,
           out_ref, kc_ref, vc_ref,
           hid, gain_a, gain_m, cos_t, sin_t, wq, wkv, raw, wo, slots, xg, acc, qs, ob, ub,
           pbuf, dbuf, leg_out, leg_in, ffd_out, ffs_out, fin_a, fin_b, mid, res,
           sem_small, sem_raw, sem_wq, sem_wo, sem_slot, sem_down,
           ag_send, ag_recv, rs_send, rs_recv):
    t = lax.axis_index("tp")
    c = t % 2
    x = t // 2
    n_chip = lax.axis_size("tp") // 2
    xf = (x + 1 + 2 * c) % n_chip
    xs = (x + 3 + 2 * c) % n_chip
    xo = (x + 2) % n_chip
    peer = 2 * x + 1 - c
    dev_f = 2 * xf + c
    dev_s = 2 * xs + c
    rows, width = hid.shape
    heads, depth, hd = wq.shape
    tokens = xg.shape[0]
    ff = ub.shape[1]
    n_chunk = width // KC

    def local(src, dst, sem):
        return pltpu.make_async_copy(src, dst, sem)

    small = [local(hid_hbm, hid, sem_small.at[0]), local(an_hbm, gain_a, sem_small.at[1]),
             local(mn_hbm, gain_m, sem_small.at[2]), local(cos_hbm, cos_t, sem_small.at[3]),
             local(sin_hbm, sin_t, sem_small.at[4])]
    for cp in small:
        cp.start()
    pair = x
    n_raw = depth // RAW

    def raw_copies(i):
        rng = pl.ds(i * RAW, RAW)
        return [local(wk_hbm.at[rng, pair], raw.at[i % 2, 0], sem_raw.at[i % 2, 0]),
                local(wv_hbm.at[rng, pair], raw.at[i % 2, 1], sem_raw.at[i % 2, 1])]

    for i in range(2):
        for cp in raw_copies(i):
            cp.start()
    wq_copy = local(wq_hbm, wq, sem_wq)
    wq_copy.start()
    wo_copy = local(wo_hbm, wo, sem_wo)
    wo_copy.start()
    def gu_copy(i):
        src = (wg_hbm, wu_hbm)[i % 2]
        return local(src.at[pl.ds((i // 2) * KC, KC)], slots.at[i % N_SLOTS], sem_slot.at[i])
    for i in range(N_SLOTS):
        gu_copy(i).start()

    barrier = pltpu.get_barrier_semaphore()
    for dev in (peer, dev_f, dev_s):
        pl.semaphore_signal(barrier, inc=1, device_id={"tp": dev}, device_id_type=pl.DeviceIdType.MESH)

    def remote(src, dst, ssem, rsem, dev):
        return pltpu.make_async_remote_copy(src_ref=src, dst_ref=dst, send_sem=ssem, recv_sem=rsem,
                                            device_id={"tp": dev}, device_id_type=pl.DeviceIdType.MESH)

    def block(b, k):
        return xg.at[pl.ds(pl.multiple_of(b * rows, rows), rows), pl.ds(k * KC, KC)]

    def ag_copy(g, k, j):
        b, dev = [(t, dev_f), (t, dev_s), (t, peer), (dev_s, dev_f), (dev_s, peer), (dev_f, peer),
                  (2 * xo + c, peer)][j]
        return remote(block(b, k), block(b, k), ag_send.at[g, k, j], ag_recv.at[g, k, j], dev)

    def ag_arrival(g, k, j):
        b = [dev_s, dev_f, peer, 2 * xo + c, 2 * xs + 1 - c, 2 * xf + 1 - c, 2 * xo + 1 - c]
        b[4], b[5] = b[5], b[4]
        return remote(block(b[j], k), block(b[j], k), ag_send.at[g, k, j], ag_recv.at[g, k, j], peer)

    def ag_own(g, k):
        for j in range(3):
            ag_copy(g, k, j).start()

    def ag_relay(g, k):
        ag_arrival(g, k, 0).wait_recv()
        ag_copy(g, k, 3).start()
        ag_copy(g, k, 4).start()
        ag_arrival(g, k, 1).wait_recv()
        ag_copy(g, k, 5).start()

    def ag_relay2(g, k):
        ag_arrival(g, k, 3).wait_recv()
        ag_copy(g, k, 6).start()

    def ag_finish(g, k):
        for j in (2, 4, 5, 6):
            ag_arrival(g, k, j).wait_recv()

    def gather(g, compute, fill=lambda n: None):
        ag_own(g, 0)
        ag_own(g, 1)
        ag_own(g, 2)
        fill(3)
        ag_relay(g, 0)
        ag_own(g, 3)
        fill(1)
        ag_relay(g, 1)
        ag_own(g, 4)
        fill(1)
        ag_relay(g, 2)
        fill(1)
        ag_relay2(g, 0)
        fill(2)
        ag_finish(g, 0)
        compute(0)
        ag_relay(g, 3)
        ag_relay2(g, 1)
        ag_relay(g, 4)
        ag_relay2(g, 2)
        ag_finish(g, 1)
        compute(1)
        ag_relay2(g, 3)
        ag_relay2(g, 4)
        for k in range(2, n_chunk):
            ag_finish(g, k)
            compute(k)
        for k in range(n_chunk):
            for j in range(7):
                ag_copy(g, k, j).wait_send()

    cuts = [(lo + a, s) for lo, w in spans(width, ff) for a, s in spans(w, 9 * 128)]

    def rs_copy(g, i, j):
        lo, size = cuts[i]
        col = pl.ds(lo, size)
        src, dst, dev = [(pbuf.at[:, 1 - c, :, col], dbuf.at[:, :, col], peer),
                         (leg_out.at[:, col], leg_in.at[:, col], dev_f),
                         (ffs_out.at[:, col], fin_b.at[:, col], dev_s),
                         (ffd_out.at[:, col], fin_a.at[:, col], dev_f)][j]
        return remote(src, dst, rs_send.at[g, i, j], rs_recv.at[g, i, j], dev)

    def reduce_scatter(g, product, lag, finish):
        n = len(cuts)

        def make(i):
            lo, size = cuts[i]
            for a, s in spans(size, 256):
                pbuf[:, :, :, lo + a:lo + a + s] = product(lo + a, s).astype(BF).reshape(tokens // (2 * rows), 2, rows, s)
            rs_copy(g, i, 0).start()

        def chip_sum(d, lo, size):
            return pbuf[d, c, :, lo:lo + size].astype(F32) + dbuf[d, :, lo:lo + size].astype(F32)

        def combine(i):
            lo, size = cuts[i]
            rs_copy(g, i, 0).wait_recv()
            leg_out[:, lo:lo + size] = chip_sum(xo, lo, size).astype(BF)
            ffs_out[:, lo:lo + size] = chip_sum(xs, lo, size).astype(BF)
            rs_copy(g, i, 1).start()
            rs_copy(g, i, 2).start()

        def relay(i):
            lo, size = cuts[i]
            rs_copy(g, i, 1).wait_recv()
            ffd_out[:, lo:lo + size] = (chip_sum(xf, lo, size) + leg_in[:, lo:lo + size].astype(F32)).astype(BF)
            rs_copy(g, i, 3).start()

        def last(i):
            lo, size = cuts[i]
            rs_copy(g, i, 2).wait_recv()
            rs_copy(g, i, 3).wait_recv()
            total = (chip_sum(x, lo, size) + fin_a[:, lo:lo + size].astype(F32)
                     + fin_b[:, lo:lo + size].astype(F32))
            finish(lo, size, total)

        for i in range(n + lag):
            if i < n:
                make(i)
            if i >= lag:
                combine(i - lag)
        for i in range(n):
            relay(i)
        for i in range(n):
            last(i)
        for i in range(n):
            for j in range(4):
                rs_copy(g, i, j).wait_send()

    def normalize(src, gain, sum_sq):
        scale = lax.rsqrt(sum_sq * (1.0 / width) + eps)
        for lo, size in spans(width, KC):
            xg[pl.ds(pl.multiple_of(t * rows, rows), rows), lo:lo + size] = (
                src[:, lo:lo + size].astype(F32) * scale * gain[:, lo:lo + size].astype(F32)).astype(BF)

    for cp in small:
        cp.wait()
    sum_sq = jnp.zeros((rows, 1), F32)
    for lo, size in spans(width, KC):
        part = hid[:, lo:lo + size].astype(F32)
        sum_sq = sum_sq + jnp.sum(part * part, axis=-1, keepdims=True)
    normalize(hid, gain_a, sum_sq)
    pl.semaphore_wait(barrier, 3)

    row = lax.broadcasted_iota(jnp.int32, (128, 256), 0)
    col = lax.broadcasted_iota(jnp.int32, (128, 256), 1)
    pick = jnp.where(col == 2 * row + c, 1.0, 0.0).astype(BF)
    todo = list(range(n_raw))

    def select_heads(count):
        for _ in range(count):
            i = todo.pop(0)
            for cp in raw_copies(i):
                cp.wait()
            for a in range(RAW // 128):
                both = jnp.concatenate([raw[i % 2, j, 128 * a:128 * a + 128].reshape(256, hd) for j in range(2)], axis=1)
                wkv[i * RAW + 128 * a:i * RAW + 128 * a + 128, :] = dot(pick, both).astype(BF)
            if i + 2 < n_raw:
                for cp in raw_copies(i + 2):
                    cp.start()

    nq = heads * hd

    def qkv(k):
        if k == 0:
            select_heads(len(todo))
            wq_copy.wait()
        r = slice(k * KC, k * KC + KC)
        a = xg[:, r]
        for h in range(0, heads, 2):
            if h + 1 < heads:
                w = jnp.concatenate([wq[h, r, :], wq[h + 1, r, :]], axis=1)
            else:
                w = wq[h, r, :]
            part = dot(a, w)
            lo, hi = h * hd, h * hd + w.shape[1]
            acc[:, lo:hi] = part if k == 0 else acc[:, lo:hi] + part
        part = dot(a, wkv[r, :])
        acc[:, nq:nq + 2 * hd] = part if k == 0 else acc[:, nq:nq + 2 * hd] + part

    gather(0, qkv, select_heads)

    def rope(v):
        return v * cos_t[...] + jnp.concatenate([v[:, hd // 2:], v[:, :hd // 2]], axis=1) * sin_t[...]

    for h in range(heads):
        qs[h * tokens:h * tokens + tokens, :] = rope(acc[:, h * hd:h * hd + hd]).astype(BF)
    k_rot = rope(acc[:, nq:nq + hd]).astype(BF)
    v_loc = acc[:, nq + hd:nq + 2 * hd].astype(BF)
    kc_ref[...] = k_rot
    vc_ref[...] = v_loc
    seen = (lax.broadcasted_iota(jnp.int32, (tokens, tokens), 1)
            <= lax.broadcasted_iota(jnp.int32, (tokens, tokens), 0))
    for h in range(heads):
        s = lax.dot_general(qs[h * tokens:h * tokens + tokens, :], k_rot, (((1,), (1,)), ((), ())),
                            preferred_element_type=F32) * (hd ** -0.5)
        s = jnp.where(seen, s, -1e30)
        e = jnp.exp(s - jnp.max(s, axis=-1, keepdims=True))
        p = (e / jnp.sum(e, axis=-1, keepdims=True)).astype(BF)
        ob[:, h * hd:h * hd + hd] = dot(p, v_loc).astype(BF)

    wo_copy.wait()
    sq = [jnp.zeros((rows, 1), F32)]

    def mid_finish(lo, size, total):
        m = (hid[:, lo:lo + size].astype(F32) + total).astype(BF)
        mid[:, lo:lo + size] = m
        m = m.astype(F32)
        sq[0] = sq[0] + jnp.sum(m * m, axis=-1, keepdims=True)

    reduce_scatter(0, lambda lo, size: dot(ob[...], wo[:, lo:lo + size]), 3, mid_finish)

    down0 = local(wd_hbm.at[pl.ds(0, nq)], wo, sem_down.at[0])
    down0.start()
    tail = [(nq, KC), (nq + KC, ff - nq - KC)]
    pieces = [(r, n, lo, s) for lo, s in spans(width, ff) for r, n in tail]
    free = [s % N_SLOTS for s in range(2 * n_chunk)][:2 * (n_chunk - 1)]
    order = [i for i in range(2 * (n_chunk - 1))][2 * n_chunk - N_SLOTS:]
    place = [(p, order[i] % N_SLOTS, i) for i, p in enumerate(pieces)]

    def piece_copy(i):
        (r, n, lo, s), slot, j = place[i]
        return local(wd_hbm.at[pl.ds(r, n), pl.ds(lo, s)], slots.at[slot, pl.ds(0, n), pl.ds(0, s)], sem_down.at[1 + j])

    normalize(mid, gain_m, sq[0])

    def gate_up(k):
        a = xg[:, k * KC:k * KC + KC]
        for half in range(2):
            i = 2 * k + half
            gu_copy(i).wait()
            for lo, s in spans(ff, 256):
                part = dot(a, slots[i % N_SLOTS, :, lo:lo + s])
                lo2 = half * ff + lo
                acc[:, lo2:lo2 + s] = part if k == 0 else acc[:, lo2:lo2 + s] + part
            if i + N_SLOTS < 2 * n_chunk:
                gu_copy(i + N_SLOTS).start()
            for j in range(len(place)):
                if order[j] == i:
                    piece_copy(j).start()

    gather(1, gate_up)

    for lo, s in spans(ff, 256):
        g = acc[:, lo:lo + s]
        ub[:, lo:lo + s] = (g * (1.0 / (1.0 + jnp.exp(-g))) * acc[:, ff + lo:ff + lo + s]).astype(BF)
    down0.wait()
    got = set()

    def down(lo, size):
        total = dot(ub[:, :nq], wo[:, lo:lo + size])
        for i, ((r, n, plo, ps), slot, j) in enumerate(place):
            if plo <= lo < plo + ps:
                if i not in got:
                    got.add(i)
                    piece_copy(i).wait()
                total = total + dot(ub[:, r:r + n], slots[slot, :n, lo - plo:lo - plo + size])
        return total

    def out_finish(lo, size, total):
        out_ref[:, lo:lo + size] = (mid[:, lo:lo + size].astype(F32) + total).astype(BF)

    reduce_scatter(1, down, 1, out_finish)


def solution(mesh):
    tp_size = mesh.shape["tp"]

    def local_layer(hidden_in, attn_norm, mlp_norm, w_query, w_key, w_value, w_out, w_gate, w_up, w_down):
        rows, width = hidden_in.shape
        tokens = rows * tp_size
        heads, hd = w_query.shape[1:]
        kv_heads = w_key.shape[1]
        ff = w_gate.shape[1]
        half = hd // 2
        freq = (1.0 / (np.float32(500000.0) ** (np.arange(half, dtype=np.float32) * np.float32(2.0 / hd)))).astype(np.float32)
        angle = (np.arange(tokens, dtype=np.float32)[:, None] * freq[None, :]).astype(np.float32)
        cos = np.cos(angle.astype(np.float64)).astype(np.float32)
        sin = np.sin(angle.astype(np.float64)).astype(np.float32)
        cos = jnp.asarray(np.concatenate([cos, cos], axis=1))
        sin = jnp.asarray(np.concatenate([-sin, sin], axis=1))
        n_cut = len([1 for _, w in spans(width, ff) for _ in spans(w, 9 * 128)])
        n_chunk = width // KC
        any_spec = pl.BlockSpec(memory_space=pl.ANY)
        vmem = pl.BlockSpec(memory_space=pltpu.VMEM)
        row_buf = pltpu.VMEM((rows, width), BF)
        dma = pltpu.SemaphoreType.DMA
        out, k_cache, v_cache = pl.pallas_call(
            functools.partial(kernel, 1e-5),
            out_shape=(jax.ShapeDtypeStruct((rows, width), BF), jax.ShapeDtypeStruct((tokens, hd), BF),
                       jax.ShapeDtypeStruct((tokens, hd), BF)),
            in_specs=[any_spec] * 12,
            out_specs=(vmem, vmem, vmem),
            scratch_shapes=[
                row_buf, pltpu.VMEM((1, width), BF), pltpu.VMEM((1, width), BF),
                pltpu.VMEM((tokens, hd), F32), pltpu.VMEM((tokens, hd), F32),
                pltpu.VMEM((heads, width, hd), BF), pltpu.VMEM((width, 2 * hd), BF),
                pltpu.VMEM((2, 2, RAW, 2, hd), BF), pltpu.VMEM((heads * hd, width), BF),
                pltpu.VMEM((N_SLOTS, KC, ff), BF), pltpu.VMEM((tokens, width), BF),
                pltpu.VMEM((tokens, 2 * ff), F32), pltpu.VMEM((heads * tokens, hd), BF),
                pltpu.VMEM((tokens, heads * hd), BF), pltpu.VMEM((tokens, ff), BF),
                pltpu.VMEM((tp_size // 2, 2, rows, width), BF), pltpu.VMEM((tp_size // 2, rows, width), BF),
                row_buf, row_buf, row_buf, row_buf, row_buf, row_buf, row_buf, pltpu.VMEM((8, 128), F32),
                dma((5,)), dma((2, 2)), dma(()), dma(()), dma((2 * n_chunk,)), dma((8,)),
                dma((2, n_chunk, 7)), dma((2, n_chunk, 7)), dma((2, n_cut, 4)), dma((2, n_cut, 4)),
            ],
            compiler_params=pltpu.CompilerParams(collective_id=0, has_side_effects=True, vmem_limit_bytes=67_043_328),
        )(hidden_in, attn_norm.reshape(1, width), mlp_norm.reshape(1, width), cos, sin,
          jnp.transpose(w_query, (1, 0, 2)), w_key.reshape(width, kv_heads // 2, 2, hd),
          w_value.reshape(width, kv_heads // 2, 2, hd), w_out.reshape(heads * hd, width), w_gate, w_up, w_down)
        return out, k_cache.reshape(tokens, 1, hd), v_cache.reshape(tokens, 1, hd)

    row_spec = P(("dp", "tp"), None)
    cache_spec = P("dp", "tp", None)
    return jax.shard_map(local_layer, mesh=mesh, in_specs=(row_spec, P(), P(), P(None, "tp", None), P(), P(), P("tp", None, None), P(None, "tp"), P(None, "tp"), P("tp", None)), out_specs=(row_spec, cache_spec, cache_spec), check_vma=False)
```

```python
import functools

import jax
import jax.numpy as jnp
import numpy as np
from jax import lax
from jax.experimental import pallas as pl
from jax.experimental.pallas import tpu as pltpu
from jax.sharding import PartitionSpec as P

BF = jnp.bfloat16
F32 = jnp.float32
KC = 1024
RAW = 640
N_SLOTS = 9


def dot(a, b):
    return jnp.dot(a, b, preferred_element_type=F32)


def spans(width, step):
    return [(lo, min(step, width - lo)) for lo in range(0, width, step)]


def kernel(eps, hid_hbm, an_hbm, mn_hbm, cos_hbm, sin_hbm, wq_hbm, wk_hbm, wv_hbm, wo_hbm, wg_hbm, wu_hbm, wd_hbm,
           out_ref, kc_ref, vc_ref,
           hid, gain_a, gain_m, cos_t, sin_t, wq, wkv, wo, slots, xg, qacc, qs, ob,
           dbuf, leg_in, fin_a, fin_b, mid,
           sem_small, sem_raw, sem_wq, sem_wo, sem_slot, sem_down,
           ag_send, ag_recv, rs_send, rs_recv):
    t = lax.axis_index("tp")
    c = t % 2
    x = t // 2
    n_chip = lax.axis_size("tp") // 2
    xf = (x + 1 + 2 * c) % n_chip
    xs = (x + 3 + 2 * c) % n_chip
    xo = (x + 2) % n_chip
    peer = 2 * x + 1 - c
    dev_f = 2 * xf + c
    dev_s = 2 * xs + c
    rows, width = hid.shape
    heads, depth, hd = wq.shape
    tokens = xg.shape[0]
    ff = slots.shape[2]
    n_chunk = width // KC

    def local(src, dst, sem):
        return pltpu.make_async_copy(src, dst, sem)

    small = [local(hid_hbm, hid, sem_small.at[0]), local(an_hbm, gain_a, sem_small.at[1]),
             local(mn_hbm, gain_m, sem_small.at[2]), local(cos_hbm, cos_t, sem_small.at[3]),
             local(sin_hbm, sin_t, sem_small.at[4])]
    for cp in small:
        cp.start()
    pair = x
    n_raw = depth // RAW

    wq_copy = local(wq_hbm, wq, sem_wq)
    wo_copy = local(wo_hbm, wo, sem_wo)

    def gu_copy(i):
        src = (wg_hbm, wu_hbm)[i % 2]
        return local(src.at[pl.ds((i // 2) * KC, KC)], slots.at[i % N_SLOTS], sem_slot.at[i])

    def remote(src, dst, ssem, rsem, dev):
        return pltpu.make_async_remote_copy(src_ref=src, dst_ref=dst, send_sem=ssem, recv_sem=rsem,
                                            device_id={"tp": dev}, device_id_type=pl.DeviceIdType.MESH)

    def block(b, k):
        return xg.at[pl.ds(pl.multiple_of(b * rows, rows), rows), pl.ds(k * KC, KC)]

    def ag_copy(g, k, j):
        b, dev = [(t, dev_f), (t, dev_s), (t, peer), (dev_s, dev_f), (dev_s, peer), (dev_f, peer),
                  (2 * xo + c, peer)][j]
        return remote(block(b, k), block(b, k), ag_send.at[g, k, j], ag_recv.at[g, k, j], dev)

    def ag_arrival(g, k, j):
        b = [dev_s, dev_f, peer, 2 * xo + c, 2 * xs + 1 - c, 2 * xf + 1 - c, 2 * xo + 1 - c]
        b[4], b[5] = b[5], b[4]
        return remote(block(b[j], k), block(b[j], k), ag_send.at[g, k, j], ag_recv.at[g, k, j], peer)

    def ag_own(g, k):
        for j in range(3):
            ag_copy(g, k, j).start()

    def ag_relay(g, k):
        ag_arrival(g, k, 0).wait_recv()
        ag_copy(g, k, 3).start()
        ag_copy(g, k, 4).start()
        ag_arrival(g, k, 1).wait_recv()
        ag_copy(g, k, 5).start()

    def ag_relay2(g, k):
        ag_arrival(g, k, 3).wait_recv()
        ag_copy(g, k, 6).start()

    def ag_finish(g, k):
        for j in (2, 4, 5, 6):
            ag_arrival(g, k, j).wait_recv()

    def gather(g, compute, fill=lambda n: None):
        ag_own(g, 0)
        ag_own(g, 1)
        ag_own(g, 2)
        fill(3)
        ag_relay(g, 0)
        ag_own(g, 3)
        fill(1)
        ag_relay(g, 1)
        ag_own(g, 4)
        fill(1)
        ag_relay(g, 2)
        fill(1)
        ag_relay2(g, 0)
        fill(2)
        ag_finish(g, 0)
        compute(0)
        ag_relay(g, 3)
        ag_relay2(g, 1)
        ag_relay(g, 4)
        ag_relay2(g, 2)
        ag_finish(g, 1)
        compute(1)
        ag_relay2(g, 3)
        ag_relay2(g, 4)
        for k in range(2, n_chunk):
            ag_finish(g, k)
            compute(k)
        for k in range(n_chunk):
            for j in range(7):
                ag_copy(g, k, j).wait_send()

    cuts = [(lo + a, s) for lo, w in spans(width, ff) for a, s in spans(w, 9 * 128)]

    def normalize(src, gain, sum_sq):
        scale = lax.rsqrt(sum_sq * (1.0 / width) + eps)
        rows_f = gain[...].astype(F32)
        for i in range(width // 128):
            cols = slice(i * 128, i * 128 + 128)
            xg[pl.ds(pl.multiple_of(t * rows, rows), rows), cols] = (
                src[:, cols].astype(F32) * scale * rows_f[i:i + 1, :]).astype(BF)

    nq = heads * hd

    def first_part(raw):
        def raw_copies(i):
            rng = pl.ds(i * RAW, RAW)
            return [local(wk_hbm.at[rng, pair], raw.at[0, rng], sem_raw.at[i, 0]),
                    local(wv_hbm.at[rng, pair], raw.at[1, rng], sem_raw.at[i, 1])]

        for i in range(n_raw):
            for cp in raw_copies(i):
                cp.start()
        wq_copy.start()
        wo_copy.start()
        for i in range(N_SLOTS):
            gu_copy(i).start()

        barrier = pltpu.get_barrier_semaphore()
        for dev in (peer, dev_f, dev_s):
            pl.semaphore_signal(barrier, inc=1, device_id={"tp": dev}, device_id_type=pl.DeviceIdType.MESH)

        for cp in small:
            cp.wait()
        sum_sq = jnp.zeros((rows, 1), F32)
        for lo, size in spans(width, KC):
            part = hid[:, lo:lo + size].astype(F32)
            sum_sq = sum_sq + jnp.sum(part * part, axis=-1, keepdims=True)
        normalize(hid, gain_a, sum_sq)
        pl.semaphore_wait(barrier, 3)

        row = lax.broadcasted_iota(jnp.int32, (128, 256), 0)
        col = lax.broadcasted_iota(jnp.int32, (128, 256), 1)
        pick = jnp.where(col == 2 * row + c, 1.0, 0.0).astype(BF)
        todo = list(range(n_raw))

        def select_heads(count):
            for _ in range(count):
                i = todo.pop(0)
                for cp in raw_copies(i):
                    cp.wait()
                for a in range(RAW // 128):
                    both = jnp.concatenate([raw[j, i * RAW + 128 * a:i * RAW + 128 * a + 128].reshape(256, hd) for j in range(2)], axis=1)
                    wkv[i * RAW + 128 * a:i * RAW + 128 * a + 128, :] = dot(pick, both).astype(BF)


        def qkv(k):
            if k == 0:
                select_heads(len(todo))
                wq_copy.wait()
            r = slice(k * KC, k * KC + KC)
            a = xg[:, r]
            for h in range(0, heads, 2):
                if h + 1 < heads:
                    w = jnp.concatenate([wq[h, r, :], wq[h + 1, r, :]], axis=1)
                else:
                    w = wq[h, r, :]
                part = dot(a, w)
                lo, hi = h * hd, h * hd + w.shape[1]
                qacc[:, lo:hi] = part if k == 0 else qacc[:, lo:hi] + part
            part = dot(a, wkv[r, :])
            qacc[:, nq:nq + 2 * hd] = part if k == 0 else qacc[:, nq:nq + 2 * hd] + part

        gather(0, qkv, select_heads)


    pl.run_scoped(first_part, pltpu.VMEM((2, depth, 2, hd), BF))

    def rope(v):
        return v * cos_t[...] + jnp.concatenate([v[:, hd // 2:], v[:, :hd // 2]], axis=1) * sin_t[...]

    for h in range(heads):
        qs[h * tokens:h * tokens + tokens, :] = rope(qacc[:, h * hd:h * hd + hd]).astype(BF)
    k_rot = rope(qacc[:, nq:nq + hd]).astype(BF)
    v_loc = qacc[:, nq + hd:nq + 2 * hd].astype(BF)
    kc_ref[...] = k_rot
    vc_ref[...] = v_loc
    seen = (lax.broadcasted_iota(jnp.int32, (tokens, tokens), 1)
            <= lax.broadcasted_iota(jnp.int32, (tokens, tokens), 0))
    for h in range(heads):
        s = lax.dot_general(qs[h * tokens:h * tokens + tokens, :], k_rot, (((1,), (1,)), ((), ())),
                            preferred_element_type=F32) * (hd ** -0.5)
        s = jnp.where(seen, s, -1e30)
        e = jnp.exp(s - jnp.max(s, axis=-1, keepdims=True))
        p = (e / jnp.sum(e, axis=-1, keepdims=True)).astype(BF)
        ob[:, h * hd:h * hd + hd] = dot(p, v_loc).astype(BF)

    def second_part(acc, ub, pbuf, leg_out, ffd_out, ffs_out):
        def rs_copy(g, i, j):
            lo, size = cuts[i]
            col = pl.ds(lo, size)
            src, dst, dev = [(pbuf.at[:, 1 - c, :, col], dbuf.at[:, :, col], peer),
                             (leg_out.at[:, col], leg_in.at[:, col], dev_f),
                             (ffs_out.at[:, col], fin_b.at[:, col], dev_s),
                             (ffd_out.at[:, col], fin_a.at[:, col], dev_f)][j]
            return remote(src, dst, rs_send.at[g, i, j], rs_recv.at[g, i, j], dev)

        def reduce_scatter(g, product, lag, finish):
            n = len(cuts)

            def make(i):
                lo, size = cuts[i]
                for a, s in spans(size, 256):
                    pbuf[:, :, :, lo + a:lo + a + s] = product(lo + a, s).astype(BF).reshape(tokens // (2 * rows), 2, rows, s)
                rs_copy(g, i, 0).start()

            def chip_sum(d, lo, size):
                return pbuf[d, c, :, lo:lo + size].astype(F32) + dbuf[d, :, lo:lo + size].astype(F32)

            def combine(i):
                lo, size = cuts[i]
                rs_copy(g, i, 0).wait_recv()
                leg_out[:, lo:lo + size] = chip_sum(xo, lo, size).astype(BF)
                ffs_out[:, lo:lo + size] = chip_sum(xs, lo, size).astype(BF)
                rs_copy(g, i, 1).start()
                rs_copy(g, i, 2).start()

            def relay(i):
                lo, size = cuts[i]
                rs_copy(g, i, 1).wait_recv()
                ffd_out[:, lo:lo + size] = (chip_sum(xf, lo, size) + leg_in[:, lo:lo + size].astype(F32)).astype(BF)
                rs_copy(g, i, 3).start()

            def last(i):
                lo, size = cuts[i]
                rs_copy(g, i, 2).wait_recv()
                rs_copy(g, i, 3).wait_recv()
                total = (chip_sum(x, lo, size) + fin_a[:, lo:lo + size].astype(F32)
                         + fin_b[:, lo:lo + size].astype(F32))
                finish(lo, size, total)

            for i in range(n + lag):
                if i < n:
                    make(i)
                if i >= lag:
                    combine(i - lag)
            for i in range(n):
                relay(i)
            for i in range(n):
                last(i)
            for i in range(n):
                for j in range(4):
                    rs_copy(g, i, j).wait_send()

        wo_copy.wait()
        sq = [jnp.zeros((rows, 1), F32)]

        def mid_finish(lo, size, total):
            m = (hid[:, lo:lo + size].astype(F32) + total).astype(BF)
            mid[:, lo:lo + size] = m
            m = m.astype(F32)
            sq[0] = sq[0] + jnp.sum(m * m, axis=-1, keepdims=True)

        reduce_scatter(0, lambda lo, size: dot(ob[...], wo[:, lo:lo + size]), 3, mid_finish)

        down0 = local(wd_hbm.at[pl.ds(0, nq)], wo, sem_down.at[0])
        down0.start()
        tail = [(nq, KC), (nq + KC, ff - nq - KC)]
        pieces = [(r, n, lo, s) for lo, s in spans(width, ff) for r, n in tail]
        free = [s % N_SLOTS for s in range(2 * n_chunk)][:2 * (n_chunk - 1)]
        order = [i for i in range(2 * (n_chunk - 1))][2 * n_chunk - N_SLOTS:]
        place = [(p, order[i] % N_SLOTS, i) for i, p in enumerate(pieces)]

        def piece_copy(i):
            (r, n, lo, s), slot, j = place[i]
            return local(wd_hbm.at[pl.ds(r, n), pl.ds(lo, s)], slots.at[slot, pl.ds(0, n), pl.ds(0, s)], sem_down.at[1 + j])

        normalize(mid, gain_m, sq[0])

        def gate_up(k):
            a = xg[:, k * KC:k * KC + KC]
            for half in range(2):
                i = 2 * k + half
                gu_copy(i).wait()
                for lo, s in spans(ff, 256):
                    part = dot(a, slots[i % N_SLOTS, :, lo:lo + s])
                    lo2 = half * ff + lo
                    acc[:, lo2:lo2 + s] = part if k == 0 else acc[:, lo2:lo2 + s] + part
                if i + N_SLOTS < 2 * n_chunk:
                    gu_copy(i + N_SLOTS).start()
                for j in range(len(place)):
                    if order[j] == i:
                        piece_copy(j).start()

        gather(1, gate_up)

        for lo, s in spans(ff, 256):
            g = acc[:, lo:lo + s]
            ub[:, lo:lo + s] = (g * (1.0 / (1.0 + jnp.exp(-g))) * acc[:, ff + lo:ff + lo + s]).astype(BF)
        down0.wait()
        got = set()

        def down(lo, size):
            total = dot(ub[:, :nq], wo[:, lo:lo + size])
            for i, ((r, n, plo, ps), slot, j) in enumerate(place):
                if plo <= lo < plo + ps:
                    if i not in got:
                        got.add(i)
                        piece_copy(i).wait()
                    total = total + dot(ub[:, r:r + n], slots[slot, :n, lo - plo:lo - plo + size])
            return total

        def out_finish(lo, size, total):
            out_ref[:, lo:lo + size] = (mid[:, lo:lo + size].astype(F32) + total).astype(BF)

        reduce_scatter(1, down, 1, out_finish)

    row_buf = pltpu.VMEM((rows, width), BF)
    pl.run_scoped(second_part, pltpu.VMEM((tokens, 2 * ff), F32), pltpu.VMEM((tokens, ff), BF),
                  pltpu.VMEM((n_chip, 2, rows, width), BF), row_buf, row_buf, row_buf)


def hand_over(*refs):
    n = len(refs) // 3
    src, dst, buf, sem = refs[:n], refs[n:2 * n], refs[2 * n:3 * n], refs[3 * n]
    ins = [pltpu.make_async_copy(src[i], buf[i], sem.at[0, i]) for i in range(n)]
    outs = [pltpu.make_async_copy(buf[i], dst[i], sem.at[1, i]) for i in range(n)]
    for cp in ins:
        cp.start()
    for i in range(n):
        ins[i].wait()
        outs[i].start()
    for cp in outs:
        cp.wait()


def solution(mesh):
    tp_size = mesh.shape["tp"]

    def local_layer(hidden_in, attn_norm, mlp_norm, w_query, w_key, w_value, w_out, w_gate, w_up, w_down):
        rows, width = hidden_in.shape
        tokens = rows * tp_size
        heads, hd = w_query.shape[1:]
        kv_heads = w_key.shape[1]
        ff = w_gate.shape[1]
        half = hd // 2
        freq = (1.0 / (np.float32(500000.0) ** (np.arange(half, dtype=np.float32) * np.float32(2.0 / hd)))).astype(np.float32)
        angle = (np.arange(tokens, dtype=np.float32)[:, None] * freq[None, :]).astype(np.float32)
        cos = np.cos(angle.astype(np.float64)).astype(np.float32)
        sin = np.sin(angle.astype(np.float64)).astype(np.float32)
        cos = jnp.asarray(np.concatenate([cos, cos], axis=1))
        sin = jnp.asarray(np.concatenate([-sin, sin], axis=1))
        n_cut = len([1 for _, w in spans(width, ff) for _ in spans(w, 9 * 128)])
        n_chunk = width // KC
        any_spec = pl.BlockSpec(memory_space=pl.ANY)
        vmem = pl.BlockSpec(memory_space=pltpu.VMEM)
        row_buf = pltpu.VMEM((rows, width), BF)
        dma = pltpu.SemaphoreType.DMA
        out, k_cache, v_cache = pl.pallas_call(
            functools.partial(kernel, 1e-5),
            out_shape=(jax.ShapeDtypeStruct((rows, width), BF), jax.ShapeDtypeStruct((tokens, hd), BF),
                       jax.ShapeDtypeStruct((tokens, hd), BF)),
            in_specs=[any_spec] * 12,
            out_specs=(vmem, vmem, vmem),
            scratch_shapes=[
                row_buf, pltpu.VMEM((width // 128, 128), BF), pltpu.VMEM((width // 128, 128), BF),
                pltpu.VMEM((tokens, hd), F32), pltpu.VMEM((tokens, hd), F32),
                pltpu.VMEM((heads, width, hd), BF), pltpu.VMEM((width, 2 * hd), BF),
                pltpu.VMEM((heads * hd, width), BF),
                pltpu.VMEM((N_SLOTS, KC, ff), BF), pltpu.VMEM((tokens, width), BF),
                pltpu.VMEM((tokens, (heads + 2) * hd), F32), pltpu.VMEM((heads * tokens, hd), BF),
                pltpu.VMEM((tokens, heads * hd), BF), pltpu.VMEM((tp_size // 2, rows, width), BF),
                row_buf, row_buf, row_buf, row_buf,
                dma((5,)), dma((width // RAW, 2)), dma(()), dma(()), dma((2 * n_chunk,)), dma((8,)),
                dma((2, n_chunk, 7)), dma((2, n_chunk, 7)), dma((2, n_cut, 4)), dma((2, n_cut, 4)),
            ],
            compiler_params=pltpu.CompilerParams(collective_id=0, has_side_effects=True, vmem_limit_bytes=67_043_328),
        )(hidden_in, attn_norm.reshape(width // 128, 128), mlp_norm.reshape(width // 128, 128), cos, sin,
          jnp.transpose(w_query, (1, 0, 2)), w_key.reshape(width, kv_heads // 2, 2, hd),
          w_value.reshape(width, kv_heads // 2, 2, hd), w_out.reshape(heads * hd, width), w_gate, w_up, w_down)
        results = (out, k_cache, v_cache)
        out, k_cache, v_cache = pl.pallas_call(
            hand_over,
            out_shape=tuple(jax.ShapeDtypeStruct(r.shape, r.dtype) for r in results),
            in_specs=[any_spec] * 3,
            out_specs=(any_spec,) * 3,
            scratch_shapes=[pltpu.VMEM(r.shape, r.dtype) for r in results] + [dma((2, 3))],
        )(*results)
        return out, k_cache.reshape(tokens, 1, hd), v_cache.reshape(tokens, 1, hd)

    row_spec = P(("dp", "tp"), None)
    cache_spec = P("dp", "tp", None)
    return jax.shard_map(local_layer, mesh=mesh, in_specs=(row_spec, P(), P(), P(None, "tp", None), P(), P(), P("tp", None, None), P(None, "tp"), P(None, "tp"), P("tp", None)), out_specs=(row_spec, cache_spec, cache_spec), check_vma=False)
```
